32 devices in a mesh: dp: 8 (over z, core), tensor: 4 (over y, x).
Axes of the slice: x: 2, y: 2, z: 4, core: 2. Of those that a mesh axis runs over, the one named last changes fastest.
Arguments:
- residual_in: bfloat16 [10240, 2048], P('dp'), may hold values from -6 to 6
- layer_inputs: bfloat16 [10240, 256], P('dp'), may hold values from -6 to 6
- group_ids: int32 [16], P('dp'), may hold values from 0 to 7
- cotangent: bfloat16 [10240, 2048], P('dp'), may hold values from -6 to 6
- input_gain: float32 [2048], replicated, may hold values from 0.25 to 1.75
- laurel_left: bfloat16 [2048, 64], replicated, may hold values from -0.125 to 0.125
- laurel_right: bfloat16 [64, 2048], replicated, may hold values from -0.75 to 0.75
- laurel_gain: float32 [2048], replicated, may hold values from 0.25 to 1.75
- query_weight: bfloat16 [2048, 2048], P(None, 'tensor'), may hold values from -0.125 to 0.125
- key_matrix: bfloat16 [2048, 512], replicated, may hold values from -0.125 to 0.125
- value_matrix: bfloat16 [2048, 512], replicated, may hold values from -0.125 to 0.125
- query_gain: float32 [256], replicated, may hold values from 0.25 to 1.75
- key_gain: float32 [256], replicated, may hold values from 0.25 to 1.75
- mixer_weight: bfloat16 [2048, 2048], P('tensor'), may hold values from -0.125 to 0.125
- mixer_gain: float32 [2048], replicated, may hold values from 0.25 to 1.75
- geglu_gain: float32 [2048], replicated, may hold values from 0.25 to 1.75
- gate_weight: bfloat16 [2048, 8192], P(None, 'tensor'), may hold values from -0.125 to 0.125
- up_weight: bfloat16 [2048, 8192], P(None, 'tensor'), may hold values from -0.125 to 0.125
- down_weight: bfloat16 [8192, 2048], P('tensor'), may hold values from -0.0625 to 0.0625
- output_gain: float32 [2048], replicated, may hold values from 0.25 to 1.75
- layer_gate: bfloat16 [2048, 256], replicated, may hold values from -0.125 to 0.125
- layer_project: bfloat16 [256, 2048], replicated, may hold values from -0.375 to 0.375
- layer_gain: float32 [2048], replicated, may hold values from 0.25 to 1.75
Outputs:
- output: bfloat16 [10240, 2048], P('dp')
- residual_grad: bfloat16 [10240, 2048], P('dp')
- layer_inputs_grad: bfloat16 [10240, 256], P('dp')
- input_gain_grad: float32 [2048], P('dp')
- laurel_left_grad: float32 [2048, 64], P('dp')
- laurel_right_grad: float32 [64, 2048], P(None, 'dp')
- laurel_gain_grad: float32 [2048], P('dp')
- query_weight_grad: float32 [2048, 2048], P('dp', 'tensor')
- key_weight_grad: float32 [2048, 512], P(('dp', 'tensor'))
- value_weight_grad: float32 [2048, 512], P(('dp', 'tensor'))
- query_gain_grad: float32 [256], P(('dp', 'tensor'))
- key_gain_grad: float32 [256], P(('dp', 'tensor'))
- mixer_weight_grad: float32 [2048, 2048], P('tensor', 'dp')
- mixer_gain_grad: float32 [2048], P('dp')
- geglu_gain_grad: float32 [2048], P('dp')
- gate_weight_grad: float32 [2048, 8192], P('dp', 'tensor')
- up_weight_grad: float32 [2048, 8192], P('dp', 'tensor')
- down_weight_grad: float32 [8192, 2048], P('tensor', 'dp')
- output_gain_grad: float32 [2048], P('dp')
- layer_gate_grad: float32 [2048, 256], P('dp')
- layer_project_grad: float32 [256, 2048], P(None, 'dp')
- layer_gain_grad: float32 [2048], P('dp')
The draws below stay inside these ranges and needn't reach their ends.
Inputs may be any that keep to these rules, and one draw needn't show every extreme that they name: Continuation c follows the prompt held in dp block group_ids[c]; a prompt may have no continuation or several.
All inputs are finite; a program needn't handle non-finite values.
Results may differ from the reference program's by a relative error of at most 0.025.
Values may be sent and summed in bfloat16 or wider, within the bound.
A program may use at most 320 MiB of HBM per device.

```python
from functools import partial
import jax
import jax.numpy as jnp
from jax import lax

MODEL_WIDTH = 2048
QUERY_HEADS = 8
KEY_VALUE_HEADS = 2
HEAD_SIZE = 256
FF = 8192
LR = 64
PLD = 256
P_SIZE = 1024
L = 128
CONT_DEV = 2
ROWS = 1280
TOKENS = 10240
CONTS = 16
N_DP = 8


def set_ends(drawn, rng, least, top_value):
    longest = drawn.shape.index(max(drawn.shape))
    spots = []
    for shift in (0, 1):
        where = [jax.random.randint(jax.random.fold_in(rng, axis), (), 0, length) for axis, length in enumerate(drawn.shape)]
        where[longest] = (where[longest] + shift) % drawn.shape[longest]
        spots.append(tuple(where))
    return drawn.at[spots[0]].set(least).at[spots[1]].set(top_value)


def with_spikes(values, key, source, target, shards_of, factor):
    def block_of(position):
        return (jnp.arange(values.shape[position]) // (values.shape[position] // shards_of)).reshape((-1,) + (1,) * (values.ndim - 1 - position))

    first = jax.random.permutation(key, shards_of)[block_of(target)]
    far = (block_of(target) + shards_of // 2) % shards_of
    return jnp.where((block_of(source) == first) | (block_of(source) == far), factor * values, values)


def block_levels(key, dims, pieces, least, high):
    loudness = 1.0
    for axis_at, parts in pieces:
        steps = jax.random.uniform(jax.random.fold_in(jax.random.fold_in(key, 6), axis_at), (parts,), jnp.float32, least / len(pieces), high / len(pieces))
        loudness = loudness * jnp.repeat(jnp.exp(steps), dims[axis_at] // parts).reshape((-1,) + (1,) * (len(dims) - 1 - axis_at))
    return loudness


def gaussian(own_key, shape, deviation, limit, pieces=(), kind=jnp.bfloat16):
    values = deviation * jax.random.normal(own_key, shape, jnp.float32)
    if pieces:
        values = values * block_levels(own_key, shape, pieces, -0.22, 0.18)
    return jnp.clip(values, -limit, limit).astype(kind)


def heavy_noise(stream_key, dims, deviation, bound, split, heavy, kind=jnp.bfloat16):
    entries = deviation * jax.random.normal(stream_key, dims, jnp.float32)
    if split:
        entries = entries * block_levels(stream_key, dims, split, -0.22, 0.18)
    return jnp.clip(with_spikes(entries, jax.random.fold_in(stream_key, 3), *heavy), -bound, bound).astype(kind)


def setup_inputs(seed: int = 0) -> dict:
    key_of = jax.random.split(jax.random.key(seed), 24)
    return {
        "residual_in": gaussian(key_of[0], (TOKENS, MODEL_WIDTH), 1.0, 6.0, ((0, 8),)),
        "layer_inputs": gaussian(key_of[1], (TOKENS, PLD), 1.0, 6.0, ((0, 8),)),
        "group_ids": set_ends(jax.random.randint(key_of[2], (CONTS,), 0, N_DP), jax.random.fold_in(key_of[2], 1), 0, N_DP - 1).astype(jnp.int32),
        "cotangent": heavy_noise(key_of[3], (TOKENS, MODEL_WIDTH), 1.0, 6.0, ((0, 8),), (0, 1, 8, 2.0)),
        "input_gain": jnp.clip(1.0 + 0.15 * jax.random.normal(key_of[4], (MODEL_WIDTH,), jnp.float32), 0.25, 1.75),
        "laurel_left": gaussian(key_of[5], (MODEL_WIDTH, LR), MODEL_WIDTH ** -0.5, 0.125),
        "laurel_right": gaussian(key_of[6], (LR, MODEL_WIDTH), LR ** -0.5, 0.75),
        "laurel_gain": jnp.clip(1.0 + 0.15 * jax.random.normal(key_of[7], (MODEL_WIDTH,), jnp.float32), 0.25, 1.75),
        "query_weight": gaussian(key_of[8], (MODEL_WIDTH, QUERY_HEADS * HEAD_SIZE), MODEL_WIDTH ** -0.5, 0.125, ((1, 4),)),
        "key_matrix": gaussian(key_of[9], (MODEL_WIDTH, KEY_VALUE_HEADS * HEAD_SIZE), MODEL_WIDTH ** -0.5, 0.125),
        "value_matrix": gaussian(key_of[10], (MODEL_WIDTH, KEY_VALUE_HEADS * HEAD_SIZE), MODEL_WIDTH ** -0.5, 0.125),
        "query_gain": jnp.clip(1.0 + 0.15 * jax.random.normal(key_of[11], (HEAD_SIZE,), jnp.float32), 0.25, 1.75),
        "key_gain": jnp.clip(1.0 + 0.15 * jax.random.normal(key_of[12], (HEAD_SIZE,), jnp.float32), 0.25, 1.75),
        "mixer_weight": gaussian(key_of[13], (QUERY_HEADS * HEAD_SIZE, MODEL_WIDTH), (QUERY_HEADS * HEAD_SIZE) ** -0.5, 0.125, ((0, 4),)),
        "mixer_gain": jnp.clip(1.0 + 0.15 * jax.random.normal(key_of[14], (MODEL_WIDTH,), jnp.float32), 0.25, 1.75),
        "geglu_gain": jnp.clip(1.0 + 0.15 * jax.random.normal(key_of[15], (MODEL_WIDTH,), jnp.float32), 0.25, 1.75),
        "gate_weight": gaussian(key_of[16], (MODEL_WIDTH, FF), MODEL_WIDTH ** -0.5, 0.125, ((1, 4),)),
        "up_weight": gaussian(key_of[17], (MODEL_WIDTH, FF), MODEL_WIDTH ** -0.5, 0.125, ((1, 4),)),
        "down_weight": gaussian(key_of[18], (FF, MODEL_WIDTH), FF ** -0.5, 0.0625, ((0, 4),)),
        "output_gain": jnp.clip(1.0 + 0.15 * jax.random.normal(key_of[19], (MODEL_WIDTH,), jnp.float32), 0.25, 1.75),
        "layer_gate": gaussian(key_of[20], (MODEL_WIDTH, PLD), MODEL_WIDTH ** -0.5, 0.125),
        "layer_project": gaussian(key_of[21], (PLD, MODEL_WIDTH), PLD ** -0.5, 0.375),
        "layer_gain": jnp.clip(1.0 + 0.15 * jax.random.normal(key_of[22], (MODEL_WIDTH,), jnp.float32), 0.25, 1.75),
    }


@jax.custom_vjp
def low(v):
    return lax.optimization_barrier(v.astype(jnp.bfloat16)).astype(jnp.float32)

@jax.custom_vjp
def lowered_backward(v):
    return v

def low_keep(v):
    return (low(v), None)

def low_pass(kept, grad):
    return (grad,)

def back_keep(v):
    return (v, None)

def back_low(kept, grad):
    return (low(grad),)
low.defvjp(low_keep, low_pass)
lowered_backward.defvjp(back_keep, back_low)
EPS = 1e-06
THETA = 1000000.0
INV_ROOT = 0.7071067811865476
HIGHEST = lax.Precision.HIGHEST

def rms_norm(value, gain):
    return value * lax.rsqrt(lax.optimization_barrier(jnp.mean(value * value, axis=-1, keepdims=True)) + EPS) * gain

def exact_product(left, right):
    return jnp.dot(left, right, precision=HIGHEST, preferred_element_type=jnp.float32)

def apply_rotary(values, positions):
    width = values.shape[-1]
    half = width // 2
    freqs = THETA ** (-(jnp.arange(half, dtype=jnp.float32) * 2.0 / width))
    angles = positions.astype(jnp.float32)[:, None] * freqs[None, :]
    cosine = jnp.cos(angles)[:, None, :]
    sine = jnp.sin(angles)[:, None, :]
    first = values[..., :half]
    second = values[..., half:]
    return jnp.concatenate([first * cosine - second * sine, second * cosine + first * sine], axis=-1)

def block_positions():
    prompt_part = jnp.arange(P_SIZE, dtype=jnp.int32)
    tail_part = jnp.tile(P_SIZE + jnp.arange(L, dtype=jnp.int32), CONT_DEV)
    return jnp.concatenate([prompt_part, tail_part])

def geglu(gate, other):
    return jax.nn.gelu(gate, approximate=True) * other

def attend(queries, keys, values, allowed):
    repeat = queries.shape[1] // keys.shape[1]
    keys_wide = jnp.repeat(keys, repeat, axis=1)
    values_wide = jnp.repeat(values, repeat, axis=1)
    scale = queries.shape[-1] ** (-0.5)
    scores = lowered_backward(jnp.einsum('qhd,khd->hqk', queries, keys_wide, precision=HIGHEST) * scale)
    scores = jnp.where(allowed[None], scores, -1e+30)
    probs = low(jax.nn.softmax(scores, axis=-1))
    return jnp.einsum('hqk,khd->qhd', probs, values_wide, precision=HIGHEST)

def forward(group_ids, residual, layer_inputs, input_gain, laurel_left, laurel_right, laurel_gain, query_weight, key_matrix, value_matrix, query_gain, key_gain, mixer_weight, mixer_gain, geglu_gain, gate_weight, up_weight, down_weight, output_gain, layer_gate, layer_project, layer_gain):
    grand_total = residual.shape[0]
    blocks = grand_total // ROWS
    head_number = query_gain.shape[0]
    positions = jnp.tile(block_positions(), blocks)
    normed = rms_norm(residual, input_gain)
    lowered_normed = low(normed)
    laurel_inner = low(lowered_backward(exact_product(lowered_normed, laurel_left)))
    laurel_outer = lowered_backward(exact_product(laurel_inner, laurel_right))
    queries_raw = lowered_backward(exact_product(lowered_normed, query_weight)).reshape(grand_total, QUERY_HEADS, head_number)
    unrotated_keys = lowered_backward(exact_product(lowered_normed, key_matrix)).reshape(grand_total, KEY_VALUE_HEADS, head_number)
    unrotated_values = lowered_backward(exact_product(lowered_normed, value_matrix)).reshape(grand_total, KEY_VALUE_HEADS, head_number)
    queries = low(apply_rotary(rms_norm(queries_raw, query_gain), positions))
    keys = low(apply_rotary(rms_norm(unrotated_keys, key_gain), positions))
    values = low(rms_norm(unrotated_values, 1.0))

    def split_rows(array):
        shaped = array.reshape(blocks, ROWS, array.shape[1], head_number)
        tails = shaped[:, P_SIZE:].reshape(blocks * CONT_DEV, L, array.shape[1], head_number)
        return (shaped[:, :P_SIZE], tails)
    prompt_queries, tail_queries = split_rows(queries)
    prompt_keys, tail_keys = split_rows(keys)
    prompt_values, tail_values = split_rows(values)
    causal_prompt = jnp.arange(P_SIZE)[:, None] >= jnp.arange(P_SIZE)[None, :]
    causal_tail = jnp.arange(L)[:, None] >= jnp.arange(L)[None, :]
    tail_allowed = jnp.concatenate([jnp.ones((L, P_SIZE), dtype=bool), causal_tail], axis=1)

    def prompt_block(items):
        block_queries, block_keys, block_values = items
        return attend(block_queries, block_keys, block_values, causal_prompt)

    def tail_block(items):
        block_queries, block_keys, block_values, group = items
        group = group.astype(jnp.int32)
        own_keys = lax.dynamic_index_in_dim(prompt_keys, group, 0, keepdims=False)
        own_values = lax.dynamic_index_in_dim(prompt_values, group, 0, keepdims=False)
        return attend(block_queries, jnp.concatenate([own_keys, block_keys], axis=0), jnp.concatenate([own_values, block_values], axis=0), tail_allowed)
    prompt_mixed = lax.map(jax.checkpoint(prompt_block), (prompt_queries, prompt_keys, prompt_values))
    tail_mixed = lax.map(jax.checkpoint(tail_block), (tail_queries, tail_keys, tail_values, group_ids))
    tail_mixed = tail_mixed.reshape(blocks, CONT_DEV * L, QUERY_HEADS, head_number)
    mixed = jnp.concatenate([prompt_mixed, tail_mixed], axis=1).reshape(grand_total, QUERY_HEADS * head_number)
    mixed_low = low(lowered_backward(mixed))
    attention = lowered_backward(exact_product(mixed_low, mixer_weight))
    combined = (rms_norm(attention, mixer_gain) + residual + normed + rms_norm(laurel_outer, laurel_gain)) * INV_ROOT
    dense_in = low(rms_norm(combined, geglu_gain))
    gate = lowered_backward(exact_product(dense_in, gate_weight))
    upper = lowered_backward(exact_product(dense_in, up_weight))
    activation = low(geglu(gate, upper))
    down = lowered_backward(exact_product(activation, down_weight))
    carried = combined + rms_norm(down, output_gain)
    carried_low = low(carried)
    layer_gate_out = lowered_backward(exact_product(carried_low, layer_gate))
    layer_act = low(geglu(layer_gate_out, layer_inputs))
    layer_out = lowered_backward(exact_product(layer_act, layer_project))
    return carried + rms_norm(layer_out, layer_gain)

def reference(residual_in, layer_inputs, group_ids, cotangent, input_gain, laurel_left, laurel_right, laurel_gain, query_weight, key_matrix, value_matrix, query_gain, key_gain, mixer_weight, mixer_gain, geglu_gain, gate_weight, up_weight, down_weight, output_gain, layer_gate, layer_project, layer_gain):
    inputs = (residual_in, layer_inputs, input_gain, laurel_left, laurel_right, laurel_gain, query_weight, key_matrix, value_matrix, query_gain, key_gain, mixer_weight, mixer_gain, geglu_gain, gate_weight, up_weight, down_weight, output_gain, layer_gate, layer_project, layer_gain)
    floats = [item.astype(jnp.float32) for item in inputs]
    result, pullback = jax.vjp(partial(forward, group_ids), *floats)
    grads = pullback(cotangent.astype(jnp.float32))
    return (result.astype(jnp.bfloat16), grads[0].astype(jnp.bfloat16), grads[1].astype(jnp.bfloat16), grads[2], grads[3], grads[4], grads[5], grads[6], grads[7], grads[8], grads[9], grads[10], grads[11], grads[12], grads[13], grads[14], grads[15], grads[16], grads[17], grads[18], grads[19], grads[20])
```

```python
from functools import partial

import jax
import jax.numpy as jnp
from jax import lax
from jax.sharding import PartitionSpec as P

QUERY_HEADS = 8
KEY_VALUE_HEADS = 2
P_SIZE = 1024
L = 128
CONT_DEV = 2


EPS = 1e-06
THETA = 1000000.0
INV_ROOT = 0.7071067811865476


def rms_norm(value, gain):
    return value * lax.rsqrt(jnp.mean(value * value, axis=-1, keepdims=True) + EPS) * gain


def matmul(left, right):
    return jnp.dot(left, right, preferred_element_type=jnp.float32)


def apply_rotary(values, positions):
    width = values.shape[-1]
    half = width // 2
    freqs = THETA ** (-(jnp.arange(half, dtype=jnp.float32) * 2.0 / width))
    angles = positions.astype(jnp.float32)[:, None] * freqs[None, :]
    cosine = jnp.cos(angles)[:, None, :]
    sine = jnp.sin(angles)[:, None, :]
    first = values[..., :half]
    second = values[..., half:]
    return jnp.concatenate(
        [first * cosine - second * sine, second * cosine + first * sine], axis=-1
    )


def block_positions():
    prompt_part = jnp.arange(P_SIZE, dtype=jnp.int32)
    tail_part = jnp.tile(P_SIZE + jnp.arange(L, dtype=jnp.int32), CONT_DEV)
    return jnp.concatenate([prompt_part, tail_part])


def geglu(gate, other):
    return jax.nn.gelu(gate, approximate=True) * other


def add_norm(base, branch, gain):
    return base + rms_norm(branch, gain)


def masked_scores(queries, keys, allowed):
    scale = queries.shape[-1] ** (-0.5)
    scores = jnp.einsum("qhd,kd->hqk", queries, keys, preferred_element_type=jnp.float32) * scale
    return jnp.where(allowed[None], scores, -1e30)


def attend_forward(queries, keys, values, allowed):
    scores = masked_scores(queries, keys, allowed)
    top = jnp.max(scores, axis=-1, keepdims=True)
    weights = jnp.exp(scores - top)
    totals = jnp.sum(weights, axis=-1, keepdims=True)
    probs = (weights / totals).astype(jnp.bfloat16)
    mixed = jnp.einsum("hqk,kd->qhd", probs, values, preferred_element_type=jnp.float32)
    return (mixed, top + jnp.log(totals))


def attend_backward(queries, keys, values, allowed, log_totals, grad_mixed):
    scale = queries.shape[-1] ** (-0.5)
    probs = jnp.exp(masked_scores(queries, keys, allowed) - log_totals)
    probs_low = probs.astype(jnp.bfloat16)
    grad_probs = jnp.einsum("qhd,kd->hqk", grad_mixed, values, preferred_element_type=jnp.float32)
    centre = jnp.sum(grad_probs * probs, axis=-1, keepdims=True)
    grad_scores = (probs * (grad_probs - centre)).astype(jnp.bfloat16)
    grad_queries = (
        jnp.einsum("hqk,kd->qhd", grad_scores, keys, preferred_element_type=jnp.float32) * scale
    )
    grad_keys = (
        jnp.einsum("hqk,qhd->kd", grad_scores, queries, preferred_element_type=jnp.float32) * scale
    )
    grad_values = jnp.einsum(
        "hqk,qhd->kd", probs_low, grad_mixed, preferred_element_type=jnp.float32
    )
    return (grad_queries, grad_keys, grad_values)


def hop(value, mask):
    return lax.ppermute(value, "tensor", [(place, place ^ mask) for place in range(4)])


def gather_rows(own, size):
    if size != 4:
        return [lax.all_gather(own, "tensor", axis=0, tiled=True)]
    half = own.shape[0] // 2
    first = hop(own, 1)
    second = hop(own, 2)
    third = jnp.concatenate([hop(first[:half], 2), hop(second[half:], 1)], axis=0)
    return [own, first, second, third]


def scatter_rows(parts, size):
    if size != 4:
        return lax.psum_scatter(parts[0], "tensor", scatter_dimension=0, tiled=True).astype(
            jnp.float32
        )
    half = parts[0].shape[0] // 2
    own, first, second, third = parts

    def wide(value):
        return value.astype(jnp.float32)

    def narrow(value):
        return value.astype(jnp.bfloat16)

    far_top = hop(third[:half], 1)
    far_bottom = hop(third[half:], 2)
    near_top = hop(first[:half], 1)
    near_bottom = hop(second[half:], 2)
    onward_top = narrow(wide(second[:half]) + wide(far_top))
    onward_bottom = narrow(wide(first[half:]) + wide(far_bottom))
    last_top = hop(onward_top, 2)
    last_bottom = hop(onward_bottom, 1)
    top = wide(own[:half]) + wide(near_top) + wide(last_top)
    bottom = wide(own[half:]) + wide(near_bottom) + wide(last_bottom)
    return jnp.concatenate([top, bottom], axis=0)


def split_rows(value, place, size):
    if size != 4:
        return [value]
    rows = value.shape[0] // 4
    return [
        lax.dynamic_slice_in_dim(value, jnp.bitwise_xor(place, index) * rows, rows, 0)
        for index in range(4)
    ]


def join_rows(parts, place, size):
    if size != 4:
        return parts[0]
    rows = parts[0].shape[0]
    whole = jnp.zeros((rows * 4,) + parts[0].shape[1:], parts[0].dtype)
    for index in range(4):
        whole = lax.dynamic_update_slice_in_dim(
            whole, parts[index], jnp.bitwise_xor(place, index) * rows, 0
        )
    return whole


def stack_rows(parts):
    return parts[0] if len(parts) == 1 else jnp.concatenate(parts, axis=0)


def narrow(value):
    return value.astype(jnp.bfloat16)


def scatter_sum(value, dimension):
    return lax.psum_scatter(
        narrow(value), "dp", scatter_dimension=dimension, tiled=True
    ).astype(jnp.float32)


def sum_places(value, size):
    if size != 4:
        return lax.psum(value, "tensor")
    value = value + hop(value, 1)
    return value + hop(value, 2)


def on_device(
    mesh_sizes,
    residual_in,
    layer_inputs,
    group_ids,
    cotangent,
    input_gain,
    laurel_left,
    laurel_right,
    laurel_gain,
    query_weight,
    key_matrix,
    value_matrix,
    query_gain,
    key_gain,
    mixer_weight,
    mixer_gain,
    geglu_gain,
    gate_weight,
    up_weight,
    down_weight,
    output_gain,
    layer_gate,
    layer_project,
    layer_gain,
):
    size = mesh_sizes["tensor"]
    blocks = mesh_sizes["dp"]
    place = lax.axis_index("tensor")
    rows = residual_in.shape[0]
    part_rows = rows // size
    width = residual_in.shape[1]
    head_number = query_gain.shape[0]
    device_heads = query_weight.shape[1] // head_number
    conts = group_ids.shape[0]
    key_value_index = place * device_heads // (QUERY_HEADS // KEY_VALUE_HEADS)
    positions = block_positions()

    def own_rows(value):
        return lax.dynamic_slice_in_dim(value, place * part_rows, part_rows, 0)

    lowered_normed = narrow(rms_norm(residual_in.astype(jnp.float32), input_gain))
    residual = own_rows(residual_in).astype(jnp.float32)
    extra = own_rows(layer_inputs).astype(jnp.float32)
    cotangent_own = own_rows(cotangent).astype(jnp.float32)
    normed, input_pull = jax.vjp(rms_norm, residual, input_gain)
    normed_own = narrow(normed)
    key_slice = lax.dynamic_slice_in_dim(key_matrix, key_value_index * head_number, head_number, 1)
    value_slice = lax.dynamic_slice_in_dim(
        value_matrix, key_value_index * head_number, head_number, 1
    )
    unrotated_keys = matmul(lowered_normed, key_slice)
    unrotated_values = matmul(lowered_normed, value_slice)
    queries_raw = matmul(lowered_normed, query_weight)

    def shape_keys(key_part, value_part, gain_key):
        shaped_keys = apply_rotary(rms_norm(key_part, gain_key)[:, None, :], positions)[:, 0]
        return (shaped_keys, rms_norm(value_part, 1.0))

    def shape_queries(query_part, gain_query):
        return apply_rotary(
            rms_norm(query_part.reshape(rows, device_heads, head_number), gain_query), positions
        )

    shaped_keys, keys_pull = jax.vjp(shape_keys, unrotated_keys, unrotated_values, key_gain)
    shaped_queries, queries_pull = jax.vjp(shape_queries, queries_raw, query_gain)
    queries_low = narrow(shaped_queries)
    keys_low = narrow(shaped_keys[0])
    values_low = narrow(shaped_keys[1])
    prompt_both = lax.all_gather(
        jnp.concatenate([keys_low[:P_SIZE], values_low[:P_SIZE]], axis=1), "dp", axis=0, tiled=True
    )
    span = prompt_both.shape[0]
    causal_prompt = jnp.arange(P_SIZE)[:, None] >= jnp.arange(P_SIZE)[None, :]
    causal_tail = jnp.arange(L)[:, None] >= jnp.arange(L)[None, :]
    tail_allowed = jnp.concatenate([jnp.ones((L, P_SIZE), dtype=bool), causal_tail], axis=1)
    prompt_mixed, prompt_lse = attend_forward(
        queries_low[:P_SIZE], keys_low[:P_SIZE], values_low[:P_SIZE], causal_prompt
    )

    def own_prompt(whole, group):
        return lax.dynamic_slice_in_dim(whole, group * P_SIZE, P_SIZE, 0)

    own_both = jax.vmap(own_prompt, in_axes=(None, 0))(prompt_both, group_ids)
    own_keys = own_both[:, :, :head_number]
    own_values = own_both[:, :, head_number:]
    tail_keys = jnp.concatenate(
        [own_keys, keys_low[P_SIZE:].reshape(conts, L, head_number)], axis=1
    )
    tail_values = jnp.concatenate(
        [own_values, values_low[P_SIZE:].reshape(conts, L, head_number)], axis=1
    )
    tail_queries = queries_low[P_SIZE:].reshape(conts, L, device_heads, head_number)
    tail_mixed, tail_lse = jax.vmap(attend_forward, in_axes=(0, 0, 0, None))(
        tail_queries, tail_keys, tail_values, tail_allowed
    )
    tail_mixed = tail_mixed.reshape(conts * L, device_heads, head_number)
    mixed_low = narrow(
        jnp.concatenate([prompt_mixed, tail_mixed], axis=0).reshape(
            rows, device_heads * head_number
        )
    )
    mixed_parts = split_rows(mixed_low, place, size)
    attention = scatter_rows(
        [narrow(matmul(piece, mixer_weight)) for piece in mixed_parts], size
    )
    laurel_inner = narrow(matmul(normed_own, laurel_left))
    laurel_outer = matmul(laurel_inner, laurel_right)

    def mix_all(attended, source, normed_in, outer, gain_mixer, gain_laurel):
        return (
            rms_norm(attended, gain_mixer) + source + normed_in + rms_norm(outer, gain_laurel)
        ) * INV_ROOT

    combined, mix_pull = jax.vjp(
        mix_all, attention, residual, normed, laurel_outer, mixer_gain, laurel_gain
    )
    dense_float, pre_pull = jax.vjp(rms_norm, combined, geglu_gain)
    dense_parts = gather_rows(narrow(dense_float), size)
    gate_pulls = []
    activation_parts = []
    down_parts = []
    for piece in dense_parts:
        gate = matmul(piece, gate_weight)
        upper = matmul(piece, up_weight)
        activation_float, pull = jax.vjp(geglu, gate, upper)
        gate_pulls.append(pull)
        activation_parts.append(narrow(activation_float))
        down_parts.append(narrow(matmul(activation_parts[-1], down_weight)))
    down = scatter_rows(down_parts, size)
    carried, dense_pull = jax.vjp(add_norm, combined, down, output_gain)
    carried_low = narrow(carried)
    layer_gate_out = matmul(carried_low, layer_gate)
    layer_float, layer_pull = jax.vjp(geglu, layer_gate_out, extra)
    layer_act = narrow(layer_float)
    layer_out = matmul(layer_act, layer_project)
    result, tail_pull = jax.vjp(add_norm, carried, layer_out, layer_gain)
    output_own = narrow(result)
    grad_carried, grad_layer_out, layer_gain_grad = tail_pull(cotangent_own)
    grad_layer_low = narrow(grad_layer_out)
    grad_layer_act = matmul(grad_layer_low, layer_project.T)
    grad_gate_out, grad_extra = layer_pull(grad_layer_act)
    layer_inputs_grad_own = narrow(grad_extra)
    grad_gate_low = narrow(grad_gate_out)
    grad_carried = grad_carried + matmul(grad_gate_low, layer_gate.T)
    grad_combined, grad_down, output_gain_grad = dense_pull(grad_carried)
    grad_down_parts = gather_rows(narrow(grad_down), size)
    gate_low_parts = []
    upper_low_parts = []
    dense_grad_parts = []
    for piece, pull in zip(grad_down_parts, gate_pulls):
        grad_gate, grad_upper = pull(matmul(piece, down_weight.T))
        gate_low_parts.append(narrow(grad_gate))
        upper_low_parts.append(narrow(grad_upper))
        dense_grad_parts.append(
            narrow(
                matmul(gate_low_parts[-1], gate_weight.T)
                + matmul(upper_low_parts[-1], up_weight.T)
            )
        )
    down_sum = scatter_sum(
        matmul(stack_rows(activation_parts).T, stack_rows(grad_down_parts)), 1
    )
    dense_whole = stack_rows(dense_parts)
    gate_sum = scatter_sum(matmul(dense_whole.T, stack_rows(gate_low_parts)), 0)
    up_sum = scatter_sum(matmul(dense_whole.T, stack_rows(upper_low_parts)), 0)
    grad_dense = scatter_rows(dense_grad_parts, size)
    output_own, grad_dense = lax.optimization_barrier((output_own, grad_dense))
    output = join_rows(gather_rows(output_own, size), place, size)
    layer_inputs_grad = join_rows(gather_rows(layer_inputs_grad_own, size), place, size)
    layer_gate_grad = matmul(carried_low.T, grad_gate_low)
    layer_project_grad = matmul(grad_layer_low.T, layer_act)
    grad_combined_pre, geglu_gain_grad = pre_pull(grad_dense)
    grad_combined = grad_combined + grad_combined_pre
    grad_attention, grad_source, grad_normed_mix, grad_outer, mixer_gain_grad, laurel_gain_grad = (
        mix_pull(grad_combined)
    )
    grad_attention_parts = gather_rows(narrow(grad_attention), size)
    mixer_sum = scatter_sum(
        matmul(stack_rows(mixed_parts).T, stack_rows(grad_attention_parts)), 1
    )
    grad_mixed = join_rows(
        [narrow(matmul(piece, mixer_weight.T)) for piece in grad_attention_parts], place, size
    ).reshape(rows, device_heads, head_number)
    prompt_dq, prompt_dk, prompt_dv = attend_backward(
        queries_low[:P_SIZE],
        keys_low[:P_SIZE],
        values_low[:P_SIZE],
        causal_prompt,
        prompt_lse,
        grad_mixed[:P_SIZE],
    )
    tail_dq, tail_dk, tail_dv = jax.vmap(attend_backward, in_axes=(0, 0, 0, None, 0, 0))(
        tail_queries,
        tail_keys,
        tail_values,
        tail_allowed,
        tail_lse,
        grad_mixed[P_SIZE:].reshape(conts, L, device_heads, head_number),
    )
    cont_both = jnp.concatenate([tail_dk[:, :P_SIZE], tail_dv[:, :P_SIZE]], axis=2)
    spread = jnp.zeros((span, 2 * head_number), jnp.float32)
    for index in range(conts):
        start = group_ids[index] * P_SIZE
        spread = lax.dynamic_update_slice_in_dim(
            spread,
            lax.dynamic_slice_in_dim(spread, start, P_SIZE, 0) + cont_both[index],
            start,
            0,
        )
    owner_both = scatter_sum(spread, 0)
    grad_queries = jnp.concatenate(
        [prompt_dq, tail_dq.reshape(conts * L, device_heads, head_number)], axis=0
    )
    grad_keys = jnp.concatenate(
        [
            prompt_dk + owner_both[:, :head_number],
            tail_dk[:, P_SIZE:].reshape(conts * L, head_number),
        ],
        axis=0,
    )
    grad_values = jnp.concatenate(
        [
            prompt_dv + owner_both[:, head_number:],
            tail_dv[:, P_SIZE:].reshape(conts * L, head_number),
        ],
        axis=0,
    )
    query_part, query_gain_part = queries_pull(grad_queries)
    query_low = narrow(query_part)
    query_sum = scatter_sum(matmul(lowered_normed.T, query_low), 0)
    key_part, value_part, key_gain_part = keys_pull((grad_keys, grad_values))
    both_low = jnp.concatenate([narrow(key_part), narrow(value_part)], axis=1)
    both_weight = jnp.concatenate([key_slice, value_slice], axis=1)
    both_sum = scatter_sum(matmul(lowered_normed.T, both_low), 0)
    grad_normed_heads = scatter_rows(
        [
            narrow(matmul(query_piece, query_weight.T) + matmul(both_piece, both_weight.T))
            for query_piece, both_piece in zip(
                split_rows(query_low, place, size), split_rows(both_low, place, size)
            )
        ],
        size,
    )
    grad_outer_low = narrow(grad_outer)
    laurel_right_grad = matmul(grad_outer_low.T, laurel_inner)
    grad_inner_low = narrow(matmul(grad_outer_low, laurel_right.T))
    laurel_left_grad = matmul(normed_own.T, grad_inner_low)
    grad_normed = grad_normed_heads + grad_normed_mix + matmul(grad_inner_low, laurel_left.T)
    grad_source_norm, input_gain_grad = input_pull(grad_normed)
    residual_grad = join_rows(
        gather_rows(narrow(grad_source + grad_source_norm), size), place, size
    )
    share = width // blocks

    def place_gain(part):
        pieces = part.reshape(blocks, head_number // blocks)
        padded = jnp.pad(pieces, ((0, 0), (0, share - pieces.shape[1])))
        return padded.reshape(width)

    gains = jnp.stack(
        [
            input_gain_grad,
            laurel_gain_grad,
            mixer_gain_grad,
            geglu_gain_grad,
            output_gain_grad,
            layer_gain_grad,
            place_gain(query_gain_part),
            place_gain(key_gain_part),
        ],
        axis=1,
    )
    small = jnp.concatenate(
        [
            narrow(layer_gate_grad),
            narrow(layer_project_grad),
            narrow(laurel_left_grad),
            narrow(laurel_right_grad),
            narrow(gains),
        ],
        axis=1,
    )
    small_sum = sum_places(scatter_sum(small, 0), size)
    inner = laurel_left.shape[1]
    plain = extra.shape[1]
    layer_gate_sum = small_sum[:, :plain]
    layer_project_sum = small_sum[:, plain : 2 * plain].T
    left_sum = small_sum[:, 2 * plain : 2 * plain + inner]
    right_sum = small_sum[:, 2 * plain + inner : 2 * plain + 2 * inner].T
    gain_sums = small_sum[:, 2 * plain + 2 * inner :].T
    input_sum, laurel_sum, mixer_gain_sum, geglu_sum, output_sum, layer_sum = gain_sums[:6]
    gain_piece = head_number // (blocks * size)
    query_gain_grad = lax.dynamic_slice_in_dim(gain_sums[6], place * gain_piece, gain_piece, 0)
    key_gain_grad = lax.dynamic_slice_in_dim(gain_sums[7], place * gain_piece, gain_piece, 0)
    spread_both = lax.dynamic_update_slice_in_dim(
        jnp.zeros((share, KEY_VALUE_HEADS, 2 * head_number), jnp.float32),
        both_sum[:, None, :],
        key_value_index,
        1,
    )
    both_grad = lax.psum_scatter(spread_both, "tensor", scatter_dimension=0, tiled=True)
    key_weight_grad = both_grad[:, :, :head_number].reshape(-1, KEY_VALUE_HEADS * head_number)
    value_weight_grad = both_grad[:, :, head_number:].reshape(-1, KEY_VALUE_HEADS * head_number)
    return (
        output,
        residual_grad,
        layer_inputs_grad,
        input_sum,
        left_sum,
        right_sum,
        laurel_sum,
        query_sum,
        key_weight_grad,
        value_weight_grad,
        query_gain_grad,
        key_gain_grad,
        mixer_sum,
        mixer_gain_sum,
        geglu_sum,
        gate_sum,
        up_sum,
        down_sum,
        output_sum,
        layer_gate_sum,
        layer_project_sum,
        layer_sum,
    )


def solution(mesh):
    return jax.shard_map(
        partial(on_device, dict(mesh.shape)),
        mesh=mesh,
        in_specs=(
            P("dp", None),
            P("dp", None),
            P("dp"),
            P("dp", None),
            P(),
            P(),
            P(),
            P(),
            P(None, "tensor"),
            P(),
            P(),
            P(),
            P(),
            P("tensor", None),
            P(),
            P(),
            P(None, "tensor"),
            P(None, "tensor"),
            P("tensor", None),
            P(),
            P(),
            P(),
            P(),
        ),
        out_specs=(
            P("dp", None),
            P("dp", None),
            P("dp", None),
            P("dp"),
            P("dp", None),
            P(None, "dp"),
            P("dp"),
            P("dp", "tensor"),
            P(("dp", "tensor"), None),
            P(("dp", "tensor"), None),
            P(("dp", "tensor")),
            P(("dp", "tensor")),
            P("tensor", "dp"),
            P("dp"),
            P("dp"),
            P("dp", "tensor"),
            P("dp", "tensor"),
            P("tensor", "dp"),
            P("dp"),
            P("dp", None),
            P(None, "dp"),
            P("dp"),
        ),
        check_vma=False,
    )
```
